32 devices in a mesh: child: 4 (over z), rows: 8 (over y, x, core).
Axes of the slice: x: 2, y: 2, z: 4, core: 2. Of those that a mesh axis runs over, the one named last changes fastest.
Arguments:
- omega: bfloat16 [4, 8192, 512], P('child', 'rows'), may hold values from -6 to 6
- leaf_diag: bfloat16 [4, 32, 256, 256], P('child', 'rows'), may hold values from -0.375 to 0.375
- leaf_u: bfloat16 [4, 8192, 128], P('child', 'rows'), may hold values from -0.5 to 0.5
- leaf_v: bfloat16 [4, 8192, 128], P('child', 'rows'), may hold values from -0.375 to 0.375
- coupling: bfloat16 [4, 4096, 4096], P('child', 'rows'), may hold values from -0.09375 to 0.09375
- child_map: int32 [4, 64], P('child', 'rows'), may hold values from 0 to 95, as said below
Outputs:
- parent_rows: float32 [3, 4096, 512], P(None, ('child', 'rows'))
The draws below stay inside these ranges and needn't reach their ends.
Inputs may be any that keep to these rules, and one draw needn't show every extreme that they name: `child_map`: child block b of every child maps to one of the parent blocks 3 * (b // 2), 3 * (b // 2) + 1, 3 * (b // 2) + 2, and blocks 2 k and 2 k + 1 map to two different ones of their triple, the lower first.
All inputs are finite; a program needn't handle non-finite values.
Results may differ from the reference program's by a relative error of at most 0.004.
Values may be sent and summed in bfloat16 or wider, within the bound.
A program may use at most 128 MiB of HBM per device.

```python
import jax
import jax.numpy as jnp
from jax import lax

L = 256
R = 128
S = 512
LEAF_DEV = 4
NLEAF = 32
NC = 8192
NCB = 64
PBLK_DEV = 3
N_CHILD = 4
N_ROWS = 8


def draw_child_map(key, part):
    pairs = NCB // 2
    omitted = jax.random.randint(key, (N_CHILD, pairs), 0, 3)
    first = jnp.where(omitted == 0, 1, 0)
    second = jnp.where(omitted == 2, 1, 2)
    triple = 3 * jnp.arange(pairs, dtype=jnp.int32)[None, :]
    both = jnp.stack([triple + first, triple + second], axis=2)
    return both.reshape(N_CHILD, NCB).astype(jnp.int32)


def levels(stream_key, dims, split, least, largest):
    def one(position, shards_of):
        steps = jax.random.uniform(jax.random.fold_in(jax.random.fold_in(stream_key, 6), position), (shards_of,), jnp.float32, least / len(split), largest / len(split))
        return jnp.repeat(jnp.exp(steps), dims[position] // shards_of).reshape((-1,) + (1,) * (len(dims) - position - 1))

    gain = one(*split[0])
    for cut in split[1:]:
        gain = gain * one(*cut)
    return gain


def bell_draw(key, extent, scale, reach, pieces=(), kind=jnp.bfloat16):
    result = scale * jax.random.normal(key, extent, jnp.float32)
    if pieces:
        result = result * levels(key, extent, pieces, -0.22, 0.18)
    return jnp.clip(result, -reach, reach).astype(kind)


def setup_inputs(seed: int = 0) -> dict:
    seeds = jax.random.split(jax.random.key(seed), 7)
    return {
        "omega": bell_draw(seeds[0], (N_CHILD, NC, S), 1.0, 6.0, ((0, 4), (1, 8))),
        "leaf_diag": bell_draw(seeds[1], (N_CHILD, NLEAF, L, L), L ** -0.5, 0.375, ((0, 4), (1, 8))),
        "leaf_u": bell_draw(seeds[2], (N_CHILD, NC, R), R ** -0.5, 0.5, ((0, 4), (1, 8))),
        "leaf_v": bell_draw(seeds[3], (N_CHILD, NC, R), L ** -0.5, 0.375, ((0, 4), (1, 8))),
        "coupling": bell_draw(seeds[4], (N_CHILD, NLEAF * R, NLEAF * R), (NLEAF * R) ** -0.5, 0.09375, ((0, 4), (1, 8))),
        "child_map": draw_child_map(jax.random.fold_in(seeds[6], 71), 0),
    }


def reference(omega, leaf_diag, leaf_u, leaf_v, coupling, child_map):
    block_rows = L // 2
    parent_count = 3 * LEAF_DEV * N_ROWS
    parent = jnp.zeros((parent_count, block_rows, S), jnp.float32)
    for child_index in range(N_CHILD):
        omega_leaves = omega[child_index].astype(jnp.float32).reshape(NLEAF, L, S)
        basis_in = leaf_v[child_index].astype(jnp.float32).reshape(NLEAF, L, R)
        basis_out = leaf_u[child_index].astype(jnp.float32).reshape(NLEAF, L, R)
        sampled = jnp.einsum("nlr,nls->nrs", basis_in, omega_leaves).astype(jnp.bfloat16).reshape(NLEAF * R, S)
        coupled = jnp.dot(coupling[child_index], sampled, preferred_element_type=jnp.float32).astype(jnp.bfloat16)
        coupled = lax.optimization_barrier(coupled).astype(jnp.float32).reshape(NLEAF, R, S)
        local_part = jnp.einsum("nij,njs->nis", leaf_diag[child_index].astype(jnp.float32), omega_leaves)
        local_part = local_part + jnp.einsum("nlr,nrs->nls", basis_out, coupled)
        update = lax.optimization_barrier(local_part.astype(jnp.bfloat16)).astype(jnp.float32)
        update = update.reshape(2 * NLEAF, block_rows, S)
        parent = parent.at[child_map[child_index].astype(jnp.int32)].add(update)
    parent = parent.reshape(N_ROWS, N_CHILD, PBLK_DEV, block_rows, S)
    parent = jnp.transpose(parent, (2, 1, 0, 3, 4))
    return parent.reshape(PBLK_DEV, N_CHILD * N_ROWS * block_rows, S)
```

```python
import functools

import jax
import jax.numpy as jnp
from jax import lax
from jax.experimental import pallas as pl
from jax.experimental.pallas import tpu as pltpu
from jax.sharding import PartitionSpec as P

MESH = pl.DeviceIdType.MESH
WIDTH = 128
DEPTH = 4096


def dot(a, b):
    return jnp.dot(a, b, preferred_element_type=jnp.float32)


def kernel(
    n_child, n_rows, omega_ref, v_ref, map_ref, diag_hbm, u_hbm, coupling_hbm, out_ref,
    diag, u, coupling, gathered, local_part, coupled, update, arrived, slots, slots_in,
    load_sem, ici_send, ici_recv, fwd_send, fwd_recv, core_send, core_recv,
    z_send, z_recv, map_send, map_recv,
):
    chunks = gathered.shape[0]
    leaves, leaf = diag.shape[0], diag.shape[1]
    rank = u.shape[1]
    block = leaves * rank
    half = leaf // 2
    chips = n_rows // 2
    c = lax.axis_index("child")
    r = lax.axis_index("rows")
    chip, core = r // 2, r % 2
    partner = chip * 2 + 1 - core

    forward = chips == 4
    if forward:
        x, y = chip % 2, chip // 2
        x_near = (y * 2 + 1 - x) * 2
        y_near = ((1 - y) * 2 + x) * 2
        first = x_near * (1 - core) + y_near * core
        second = y_near * (1 - core) + x_near * core
        across = ((1 - y) * 2 + 1 - x) * 2
        direct = [(second + core, second + core), (first + core, first + core)]
        other = [first + 1 - core, second + 1 - core]
    else:
        direct = [
            (((chip + d) % chips) * 2 + core, ((chip + chips - d) % chips) * 2 + core)
            for d in range(1, chips)
        ]
        other = [((chip + chips - d) % chips) * 2 + 1 - core for d in range(1, chips)]
    sources = [r] + [s for _, s in direct]
    other = [partner] + other
    if forward:
        sources.append(across + core)
        other.append(across + 1 - core)
    if n_child == 4:
        peers = [((c + 2) % 4,) * 2, (3 - c,) * 2, (c + 1 - 2 * (c % 2),) * 2]
    else:
        peers = [((c + d) % n_child, (c + n_child - d) % n_child) for d in range(1, n_child)]

    barrier = pltpu.get_barrier_semaphore()
    for to, _ in direct + [(partner, partner)]:
        pl.semaphore_signal(barrier, inc=1, device_id=(c, to), device_id_type=MESH)
    for to, _ in peers:
        pl.semaphore_signal(barrier, inc=1, device_id=(to, r), device_id_type=MESH)

    loads = [
        pltpu.make_async_copy(diag_hbm.at[0], diag, load_sem.at[0]),
        pltpu.make_async_copy(u_hbm.at[0], u, load_sem.at[1]),
        pltpu.make_async_copy(coupling_hbm.at[0], coupling, load_sem.at[2]),
    ]
    for load in loads:
        load.start()

    def rows_of(k, source):
        return gathered.at[k, pl.ds(pl.multiple_of(source * block, block), block)]

    for i in range(leaves):
        projected = lax.dot_general(
            v_ref[0, i * leaf : (i + 1) * leaf, :],
            omega_ref[0, i * leaf : (i + 1) * leaf, :],
            (((0,), (0,)), ((), ())),
            preferred_element_type=jnp.float32,
        ).astype(jnp.bfloat16)
        for k in range(chunks):
            at = pl.ds(pl.multiple_of(r * block + i * rank, rank), rank)
            gathered[k, at, :] = projected[:, k * WIDTH : (k + 1) * WIDTH]
    for i in range(leaves):
        for b in range(2):
            slot = map_ref[0, 2 * i + b] - 3 * (r * leaves + i)
            slots[i, 8 * b : 8 * b + 8, :] = jnp.full((8, 128), slot, jnp.int32).astype(jnp.float32)

    def ici(t, k):
        return pltpu.make_async_remote_copy(
            src_ref=rows_of(k, r), dst_ref=rows_of(k, r), send_sem=ici_send.at[t, k],
            recv_sem=ici_recv.at[t, k], device_id=(c, direct[t][0]), device_id_type=MESH,
        )

    def ici_in(t, k):
        at = rows_of(k, direct[t][1])
        return pltpu.make_async_remote_copy(
            src_ref=at, dst_ref=at, send_sem=ici_send.at[t, k],
            recv_sem=ici_recv.at[t, k], device_id=(c, direct[t][0]), device_id_type=MESH,
        )

    def fwd(k):
        at = rows_of(k, direct[0][1])
        return pltpu.make_async_remote_copy(
            src_ref=at, dst_ref=at, send_sem=fwd_send.at[k],
            recv_sem=fwd_recv.at[k], device_id=(c, direct[1][0]), device_id_type=MESH,
        )

    def fwd_in(k):
        at = rows_of(k, sources[-1])
        return pltpu.make_async_remote_copy(
            src_ref=at, dst_ref=at, send_sem=fwd_send.at[k],
            recv_sem=fwd_recv.at[k], device_id=(c, direct[1][0]), device_id_type=MESH,
        )

    def across_core(t, k, who):
        at = rows_of(k, who[t])
        return pltpu.make_async_remote_copy(
            src_ref=at, dst_ref=at, send_sem=core_send.at[t, k],
            recv_sem=core_recv.at[t, k], device_id=(c, partner), device_id_type=MESH,
        )

    def to_peer(j, k):
        return pltpu.make_async_remote_copy(
            src_ref=update.at[k, peers[j][0]], dst_ref=arrived.at[j, k],
            send_sem=z_send.at[j, k], recv_sem=z_recv.at[j, k],
            device_id=(peers[j][0], r), device_id_type=MESH,
        )

    def map_to_peer(j):
        return pltpu.make_async_remote_copy(
            src_ref=slots.at[peers[j][0]], dst_ref=slots_in.at[j],
            send_sem=map_send.at[j], recv_sem=map_recv.at[j],
            device_id=(peers[j][0], r), device_id_type=MESH,
        )

    sent = []

    def start(copy):
        copy.start()
        sent.append(copy)

    def send_own(k):
        for t in range(len(direct)):
            start(ici(t, k))
        start(across_core(0, k, sources))

    def relay(k):
        for t in range(len(direct)):
            ici_in(t, k).wait_recv()
            if forward and t == 0:
                start(fwd(k))
            start(across_core(t + 1, k, sources))
        if k + 1 < chunks:
            send_own(k + 1)

    def multiply(k):
        if forward:
            fwd_in(k).wait_recv()
            start(across_core(len(sources) - 1, k, sources))
        for t in range(len(sources)):
            across_core(t, k, other).wait_recv()
        depth = gathered.shape[1]
        piece = min(DEPTH, depth)
        total = dot(coupling[:, :piece], gathered[k, :piece, :])
        if depth > piece:
            def more(b, acc):
                at = pl.ds(pl.multiple_of(b * piece, piece), piece)
                return acc + dot(coupling[:, at], gathered[k, at, :])

            total = lax.fori_loop(1, depth // piece, more, total)
        coupled[...] = total.astype(jnp.bfloat16)
        for i in range(leaves):
            rows = slice(i * leaf, (i + 1) * leaf)
            value = local_part[rows, k * WIDTH : (k + 1) * WIDTH] + dot(
                u[rows, :], coupled[i * rank : (i + 1) * rank, :]
            )
            update[k, i] = value.astype(jnp.bfloat16)
        for j in range(len(peers)):
            start(to_peer(j, k))

    def combine(k):
        totals = None
        for j in range(-1, len(peers)):
            if j < 0:
                value, where = update[k, c], slots[c]
            else:
                to_peer(j, k).wait_recv()
                value, where = arrived[j, k], slots_in[j]
            value = value.astype(jnp.float32)
            low, high = value[:half], value[half:]
            s0 = jnp.broadcast_to(where[0:1, :], low.shape)
            s1 = jnp.broadcast_to(where[8:9, :], low.shape)
            terms = [
                jnp.where(s0 == float(q), low, jnp.where(s1 == float(q), high, 0.0))
                for q in range(3)
            ]
            totals = terms if totals is None else [a + b for a, b in zip(totals, terms)]
        for q in range(3):
            out_ref[q, :, k * WIDTH : (k + 1) * WIDTH] = totals[q]

    pl.semaphore_wait(barrier, len(direct) + 1 + len(peers))
    send_own(0)
    for j in range(len(peers)):
        start(map_to_peer(j))
    loads[0].wait()
    loads[1].wait()
    for i in range(leaves):
        rows = slice(i * leaf, (i + 1) * leaf)
        local_part[rows, :] = dot(diag[i], omega_ref[0, rows, :])
    relay(0)
    loads[2].wait()
    for k in range(chunks):
        if k + 1 < chunks:
            relay(k + 1)
        multiply(k)
    for j in range(len(peers)):
        map_to_peer(j).wait_recv()
    for k in range(chunks):
        combine(k)
    for copy in sent:
        copy.wait_send()


def solution(mesh):
    n_child, n_rows = mesh.shape["child"], mesh.shape["rows"]

    def on_device(omega, leaf_diag, leaf_u, leaf_v, coupling, child_map):
        leaves, leaf = leaf_diag.shape[1], leaf_diag.shape[2]
        rank, samples = leaf_u.shape[2], omega.shape[2]
        chunks = samples // WIDTH
        block, depth = coupling.shape[1], coupling.shape[2]
        chips = n_rows // 2
        direct = 2 if chips == 4 else chips - 1
        everyone = 1 + direct + (chips == 4)
        peers = n_child - 1
        vmem = pltpu.VMEM
        bf16, f32 = jnp.bfloat16, jnp.float32
        dma = pltpu.SemaphoreType.DMA
        in_vmem = pl.BlockSpec(memory_space=pltpu.VMEM)
        anywhere = pl.BlockSpec(memory_space=pl.ANY)
        return pl.pallas_call(
            functools.partial(kernel, n_child, n_rows),
            out_shape=jax.ShapeDtypeStruct((3, leaf // 2, samples), f32),
            in_specs=[in_vmem, in_vmem, pl.BlockSpec(memory_space=pltpu.SMEM)] + [anywhere] * 3,
            out_specs=in_vmem,
            scratch_shapes=[
                vmem((leaves, leaf, leaf), bf16),
                vmem((leaves * leaf, rank), bf16),
                vmem((block, depth), bf16),
                vmem((chunks, depth, WIDTH), bf16),
                vmem((leaves * leaf, samples), f32),
                vmem((block, WIDTH), bf16),
                vmem((chunks, leaves, leaf, WIDTH), bf16),
                vmem((peers, chunks, leaf, WIDTH), bf16),
                vmem((leaves, 16, 128), f32),
                vmem((peers, 16, 128), f32),
                dma((3,)),
                dma((direct, chunks)),
                dma((direct, chunks)),
                dma((chunks,)),
                dma((chunks,)),
                dma((everyone, chunks)),
                dma((everyone, chunks)),
                dma((peers, chunks)),
                dma((peers, chunks)),
                dma((peers,)),
                dma((peers,)),
            ],
            compiler_params=pltpu.CompilerParams(
                collective_id=0, has_side_effects=True, vmem_limit_bytes=60000 * 1024
            ),
        )(omega, leaf_v, child_map, leaf_diag, leaf_u, coupling)

    placed = (
        P("child", "rows", None),
        P("child", "rows", None, None),
        P("child", "rows", None),
        P("child", "rows", None),
        P("child", "rows", None),
        P("child", "rows"),
    )
    return jax.shard_map(
        on_device,
        mesh=mesh,
        in_specs=placed,
        out_specs=P(None, ("child", "rows"), None),
        check_vma=False,
    )
```

```python
import functools

import jax
import jax.numpy as jnp
from jax import lax
from jax.experimental import pallas as pl
from jax.experimental.pallas import tpu as pltpu
from jax.sharding import PartitionSpec as P

MESH = pl.DeviceIdType.MESH
WIDTH = 128
DEPTH = 4096
STEPS = 2


def dot(a, b):
    return jnp.dot(a, b, preferred_element_type=jnp.float32)


def kernel(
    n_child, n_rows, omega_hbm, v_hbm, map_ref, diag_hbm, u_hbm, coupling_hbm, arrived, slots_in,
    omega, v, diag, u, coupling, gathered, local_part, total, coupled, update, slots,
    load_sem, ici_send, ici_recv, fwd_send, fwd_recv, core_send, core_recv,
    z_send, z_recv, map_send, map_recv, keep_sem,
):
    chunks = gathered.shape[0]
    leaves, leaf = diag.shape[0], diag.shape[1]
    rank = u.shape[1]
    block = leaves * rank
    chips = n_rows // 2
    c = lax.axis_index("child")
    r = lax.axis_index("rows")
    chip, core = r // 2, r % 2
    partner = chip * 2 + 1 - core

    forward = chips == 4
    if forward:
        x, y = chip % 2, chip // 2
        x_near = (y * 2 + 1 - x) * 2
        y_near = ((1 - y) * 2 + x) * 2
        first = x_near * (1 - core) + y_near * core
        second = y_near * (1 - core) + x_near * core
        across = ((1 - y) * 2 + 1 - x) * 2
        direct = [(second + core, second + core), (first + core, first + core)]
        other = [first + 1 - core, second + 1 - core]
    else:
        direct = [
            (((chip + d) % chips) * 2 + core, ((chip + chips - d) % chips) * 2 + core)
            for d in range(1, chips)
        ]
        other = [((chip + chips - d) % chips) * 2 + 1 - core for d in range(1, chips)]
    sources = [r] + [s for _, s in direct]
    other = [partner] + other
    if forward:
        sources.append(across + core)
        other.append(across + 1 - core)
    if n_child == 4:
        peers = [((c + 2) % 4,) * 2, (3 - c,) * 2, (c + 1 - 2 * (c % 2),) * 2]
    else:
        peers = [((c + d) % n_child, (c + n_child - d) % n_child) for d in range(1, n_child)]

    barrier = pltpu.get_barrier_semaphore()
    for to, _ in direct + [(partner, partner)]:
        pl.semaphore_signal(barrier, inc=1, device_id=(c, to), device_id_type=MESH)
    for to, _ in peers:
        pl.semaphore_signal(barrier, inc=1, device_id=(to, r), device_id_type=MESH)

    loads = [
        pltpu.make_async_copy(v_hbm.at[0], v, load_sem.at[0]),
        pltpu.make_async_copy(
            omega_hbm.at[0, :, :WIDTH], omega.at[:, :WIDTH], load_sem.at[1]
        ),
        pltpu.make_async_copy(
            omega_hbm.at[0, :, WIDTH:], omega.at[:, WIDTH:], load_sem.at[2]
        ),
        pltpu.make_async_copy(coupling_hbm.at[0], coupling, load_sem.at[3]),
        pltpu.make_async_copy(diag_hbm.at[0], diag, load_sem.at[4]),
        pltpu.make_async_copy(u_hbm.at[0], u, load_sem.at[5]),
    ]
    for load in loads:
        load.start()

    def rows_of(k, source):
        return gathered.at[k, pl.ds(pl.multiple_of(source * block, block), block)]

    def project(first, last):
        for i in range(leaves):
            rows = slice(i * leaf, (i + 1) * leaf)
            projected = lax.dot_general(
                v[rows, :],
                omega[rows, first * WIDTH : last * WIDTH],
                (((0,), (0,)), ((), ())),
                preferred_element_type=jnp.float32,
            ).astype(jnp.bfloat16)
            at = pl.ds(pl.multiple_of(r * block + i * rank, rank), rank)
            for k in range(first, last):
                gathered[k, at, :] = projected[:, (k - first) * WIDTH : (k - first + 1) * WIDTH]

    for i in range(leaves):
        for b in range(2):
            slot = map_ref[0, 2 * i + b] - 3 * (r * leaves + i)
            slots[i, 4 * b : 4 * b + 4, :] = jnp.full(
                (4, slots.shape[2]), slot, jnp.int32
            ).astype(jnp.float32)

    def ici(t, k):
        return pltpu.make_async_remote_copy(
            src_ref=rows_of(k, r), dst_ref=rows_of(k, r), send_sem=ici_send.at[t, k],
            recv_sem=ici_recv.at[t, k], device_id=(c, direct[t][0]), device_id_type=MESH,
        )

    def ici_in(t, k):
        at = rows_of(k, direct[t][1])
        return pltpu.make_async_remote_copy(
            src_ref=at, dst_ref=at, send_sem=ici_send.at[t, k],
            recv_sem=ici_recv.at[t, k], device_id=(c, direct[t][0]), device_id_type=MESH,
        )

    def fwd(k):
        at = rows_of(k, direct[0][1])
        return pltpu.make_async_remote_copy(
            src_ref=at, dst_ref=at, send_sem=fwd_send.at[k],
            recv_sem=fwd_recv.at[k], device_id=(c, direct[1][0]), device_id_type=MESH,
        )

    def fwd_in(k):
        at = rows_of(k, sources[-1])
        return pltpu.make_async_remote_copy(
            src_ref=at, dst_ref=at, send_sem=fwd_send.at[k],
            recv_sem=fwd_recv.at[k], device_id=(c, direct[1][0]), device_id_type=MESH,
        )

    def across_core(t, k, who):
        at = rows_of(k, who[t])
        return pltpu.make_async_remote_copy(
            src_ref=at, dst_ref=at, send_sem=core_send.at[t, k],
            recv_sem=core_recv.at[t, k], device_id=(c, partner), device_id_type=MESH,
        )

    def to_peer(j, k):
        return pltpu.make_async_remote_copy(
            src_ref=update.at[k, peers[j][0]], dst_ref=arrived.at[j, :, k * WIDTH : (k + 1) * WIDTH],
            send_sem=z_send.at[j, k], recv_sem=z_recv.at[j, k],
            device_id=(peers[j][0], r), device_id_type=MESH,
        )

    def map_to_peer(j):
        return pltpu.make_async_remote_copy(
            src_ref=slots.at[peers[j][0]], dst_ref=slots_in.at[j],
            send_sem=map_send.at[j], recv_sem=map_recv.at[j],
            device_id=(peers[j][0], r), device_id_type=MESH,
        )

    sent = []

    def start(copy):
        copy.start()
        sent.append(copy)

    def send_own(k):
        for t in range(len(direct)):
            start(ici(t, k))
        start(across_core(0, k, sources))

    def relay(k):
        for t in range(len(direct)):
            ici_in(t, k).wait_recv()
            if forward and t == 0:
                start(fwd(k))
            start(across_core(t + 1, k, sources))

    def keep(k):
        return pltpu.make_async_copy(
            update.at[k, c], arrived.at[len(peers), :, k * WIDTH : (k + 1) * WIDTH],
            keep_sem.at[k],
        )

    def part(k, source):
        at = pl.ds(pl.multiple_of(source * block, block), block)
        return dot(coupling[:, at], gathered[k, at, :])

    def last_arrivals(k):
        if forward:
            fwd_in(k).wait_recv()
            start(across_core(len(sources) - 1, k, sources))

    def multiply_as_it_comes(k):
        ready = sources[: len(direct) + 1]
        total[...] = part(k, ready[0])
        for source in ready[1:]:
            total[...] += part(k, source)
        for t in range(len(direct) + 1):
            across_core(t, k, other).wait_recv()
            total[...] += part(k, other[t])
        last_arrivals(k)
        if forward:
            total[...] += part(k, sources[-1])
            across_core(len(other) - 1, k, other).wait_recv()
            total[...] += part(k, other[-1])
        coupled[...] = total[...].astype(jnp.bfloat16)

    def multiply(k):
        last_arrivals(k)
        for t in range(len(sources)):
            across_core(t, k, other).wait_recv()
        depth = gathered.shape[1]
        piece = min(DEPTH, depth)
        value = dot(coupling[:, :piece], gathered[k, :piece, :])
        if depth > piece:
            def more(b, acc):
                at = pl.ds(pl.multiple_of(b * piece, piece), piece)
                return acc + dot(coupling[:, at], gathered[k, at, :])

            value = lax.fori_loop(1, depth // piece, more, value)
        coupled[...] = value.astype(jnp.bfloat16)

    def finish(k):
        for i in range(leaves):
            rows = slice(i * leaf, (i + 1) * leaf)
            value = local_part[rows, k * WIDTH : (k + 1) * WIDTH] + dot(
                u[rows, :], coupled[i * rank : (i + 1) * rank, :]
            )
            update[k, i] = value.astype(jnp.bfloat16)
        for j in range(len(peers)):
            start(to_peer(j, k))
        keep(k).start()

    loads[0].wait()
    loads[1].wait()
    project(0, 1)
    pl.semaphore_wait(barrier, len(direct) + 1 + len(peers))
    send_own(0)
    for j in range(len(peers)):
        start(map_to_peer(j))
    keep_slots = pltpu.make_async_copy(
        slots.at[c], slots_in.at[len(peers)], keep_sem.at[chunks]
    )
    keep_slots.start()
    loads[2].wait()
    if chunks > 1:
        project(1, chunks)
    for load in loads[3:]:
        load.wait()
    for i in range(leaves):
        rows = slice(i * leaf, (i + 1) * leaf)
        local_part[rows, :] = dot(diag[i], omega[rows, :])
    send_own(1)
    relay(0)
    send_own(2)
    for k in range(chunks):
        if k + 1 < chunks:
            relay(k + 1)
            if k + 3 < chunks:
                send_own(k + 3)
        ahead = [k]
        if k == 0:
            multiply_as_it_comes(k)
        else:
            multiply(k)
        if ahead[1:] and ahead[1] < chunks:
            send_own(ahead[1])
        finish(k)
    for j in range(len(peers)):
        map_to_peer(j).wait_recv()
    keep_slots.wait()
    for copy in sent:
        copy.wait_send()
    for k in range(chunks):
        keep(k).wait()
        for j in range(len(peers)):
            to_peer(j, k).wait_recv()


def combine(arrived, slots, out_ref):
    half = out_ref.shape[1]
    for j in range(arrived.shape[0]):
        value = arrived[j].astype(jnp.float32)
        low, high = value[:half], value[half:]
        s0, s1 = slots[j, 0:1, :], slots[j, 4:5, :]
        for q in range(3):
            term = jnp.where(s0 == float(q), low, jnp.where(s1 == float(q), high, 0.0))
            out_ref[q] = term if j == 0 else out_ref[q] + term


def solution(mesh):
    n_child, n_rows = mesh.shape["child"], mesh.shape["rows"]

    def on_device(omega, leaf_diag, leaf_u, leaf_v, coupling, child_map):
        leaves, leaf = leaf_diag.shape[1], leaf_diag.shape[2]
        rank, samples = leaf_u.shape[2], omega.shape[2]
        chunks = samples // WIDTH
        block, depth = coupling.shape[1], coupling.shape[2]
        chips = n_rows // 2
        direct = 2 if chips == 4 else chips - 1
        everyone = 1 + direct + (chips == 4)
        peers = n_child - 1
        vmem = pltpu.VMEM
        bf16, f32 = jnp.bfloat16, jnp.float32
        dma = pltpu.SemaphoreType.DMA
        anywhere = pl.BlockSpec(memory_space=pl.ANY)
        arrived, slots = pl.pallas_call(
            functools.partial(kernel, n_child, n_rows),
            out_shape=[
                jax.ShapeDtypeStruct((n_child, leaf, samples), bf16),
                jax.ShapeDtypeStruct((n_child, 8, samples), f32),
            ],
            in_specs=[anywhere] * 2 + [pl.BlockSpec(memory_space=pltpu.SMEM)] + [anywhere] * 3,
            out_specs=[anywhere] * 2,
            scratch_shapes=[
                vmem((leaves * leaf, samples), bf16),
                vmem((leaves * leaf, rank), bf16),
                vmem((leaves, leaf, leaf), bf16),
                vmem((leaves * leaf, rank), bf16),
                vmem((block, depth), bf16),
                vmem((chunks, depth, WIDTH), bf16),
                vmem((leaves * leaf, samples), f32),
                vmem((block, WIDTH), f32),
                vmem((block, WIDTH), bf16),
                vmem((chunks, leaves, leaf, WIDTH), bf16),
                vmem((leaves, 8, samples), f32),
                dma((6,)),
                dma((direct, chunks)),
                dma((direct, chunks)),
                dma((chunks,)),
                dma((chunks,)),
                dma((everyone, chunks)),
                dma((everyone, chunks)),
                dma((peers, chunks)),
                dma((peers, chunks)),
                dma((peers,)),
                dma((peers,)),
                dma((chunks + 1,)),
            ],
            compiler_params=pltpu.CompilerParams(
                collective_id=0, has_side_effects=True, vmem_limit_bytes=60000 * 1024
            ),
        )(omega, leaf_v, child_map, leaf_diag, leaf_u, coupling)
        width = samples // STEPS
        return pl.pallas_call(
            combine,
            grid=(STEPS,),
            out_shape=jax.ShapeDtypeStruct((3, leaf // 2, samples), f32),
            in_specs=[
                pl.BlockSpec((n_child, leaf, width), lambda i: (0, 0, i)),
                pl.BlockSpec((n_child, 8, width), lambda i: (0, 0, i)),
            ],
            out_specs=pl.BlockSpec((3, leaf // 2, width), lambda i: (0, 0, i)),
        )(arrived, slots)

    placed = (
        P("child", "rows", None),
        P("child", "rows", None, None),
        P("child", "rows", None),
        P("child", "rows", None),
        P("child", "rows", None),
        P("child", "rows"),
    )
    return jax.shard_map(
        on_device,
        mesh=mesh,
        in_specs=placed,
        out_specs=P(None, ("child", "rows"), None),
        check_vma=False,
    )
```

```python
import functools

import jax
import jax.numpy as jnp
from jax import lax
from jax.experimental import pallas as pl
from jax.experimental.pallas import tpu as pltpu
from jax.sharding import PartitionSpec as P

MESH = pl.DeviceIdType.MESH
WIDTH = 128
DEPTH = 4096
STEPS = 2


def dot(a, b):
    return jnp.dot(a, b, preferred_element_type=jnp.float32)


def kernel(
    n_child, n_rows, omega_hbm, v_hbm, map_ref, diag_hbm, u_hbm, coupling_hbm, arrived, slots_in,
    omega, v, diag, u, coupling, gathered, local_part, total, coupled, update, slots,
    load_sem, ici_send, ici_recv, fwd_send, fwd_recv, core_send, core_recv,
    z_send, z_recv, map_send, map_recv, keep_sem,
):
    chunks = gathered.shape[0]
    leaves, leaf = diag.shape[0], diag.shape[1]
    rank = u.shape[1]
    block = leaves * rank
    chips = n_rows // 2
    c = lax.axis_index("child")
    r = lax.axis_index("rows")
    chip, core = r // 2, r % 2
    partner = chip * 2 + 1 - core

    forward = chips == 4
    if forward:
        x, y = chip % 2, chip // 2
        x_near = (y * 2 + 1 - x) * 2
        y_near = ((1 - y) * 2 + x) * 2
        first = x_near * (1 - core) + y_near * core
        second = y_near * (1 - core) + x_near * core
        across = ((1 - y) * 2 + 1 - x) * 2
        direct = [(second + core, second + core), (first + core, first + core)]
        other = [first + 1 - core, second + 1 - core]
    else:
        direct = [
            (((chip + d) % chips) * 2 + core, ((chip + chips - d) % chips) * 2 + core)
            for d in range(1, chips)
        ]
        other = [((chip + chips - d) % chips) * 2 + 1 - core for d in range(1, chips)]
    sources = [r] + [s for _, s in direct]
    other = [partner] + other
    if forward:
        sources.append(across + core)
        other.append(across + 1 - core)
    if n_child == 4:
        peers = [((c + 2) % 4,) * 2, (3 - c,) * 2, (c + 1 - 2 * (c % 2),) * 2]
    else:
        peers = [((c + d) % n_child, (c + n_child - d) % n_child) for d in range(1, n_child)]

    barrier = pltpu.get_barrier_semaphore()
    for to, _ in direct + [(partner, partner)]:
        pl.semaphore_signal(barrier, inc=1, device_id=(c, to), device_id_type=MESH)
    for to, _ in peers:
        pl.semaphore_signal(barrier, inc=1, device_id=(to, r), device_id_type=MESH)

    loads = [
        pltpu.make_async_copy(v_hbm.at[0], v, load_sem.at[0]),
        pltpu.make_async_copy(
            omega_hbm.at[0, :, :WIDTH], omega.at[:, :WIDTH], load_sem.at[1]
        ),
        pltpu.make_async_copy(
            omega_hbm.at[0, :, WIDTH:], omega.at[:, WIDTH:], load_sem.at[2]
        ),
        pltpu.make_async_copy(coupling_hbm.at[0], coupling, load_sem.at[3]),
        pltpu.make_async_copy(diag_hbm.at[0], diag, load_sem.at[4]),
        pltpu.make_async_copy(u_hbm.at[0], u, load_sem.at[5]),
    ]
    for load in loads:
        load.start()

    def rows_of(k, source):
        return gathered.at[k, pl.ds(pl.multiple_of(source * block, block), block)]

    def project(first, last):
        for i in range(leaves):
            rows = slice(i * leaf, (i + 1) * leaf)
            projected = lax.dot_general(
                v[rows, :],
                omega[rows, first * WIDTH : last * WIDTH],
                (((0,), (0,)), ((), ())),
                preferred_element_type=jnp.float32,
            ).astype(jnp.bfloat16)
            at = pl.ds(pl.multiple_of(r * block + i * rank, rank), rank)
            for k in range(first, last):
                gathered[k, at, :] = projected[:, (k - first) * WIDTH : (k - first + 1) * WIDTH]

    for i in range(leaves):
        for b in range(2):
            slot = map_ref[0, 2 * i + b] - 3 * (r * leaves + i)
            slots[i, 4 * b : 4 * b + 4, :] = jnp.full(
                (4, slots.shape[2]), slot, jnp.int32
            ).astype(jnp.float32)

    def ici(t, k):
        return pltpu.make_async_remote_copy(
            src_ref=rows_of(k, r), dst_ref=rows_of(k, r), send_sem=ici_send.at[t, k],
            recv_sem=ici_recv.at[t, k], device_id=(c, direct[t][0]), device_id_type=MESH,
        )

    def ici_in(t, k):
        at = rows_of(k, direct[t][1])
        return pltpu.make_async_remote_copy(
            src_ref=at, dst_ref=at, send_sem=ici_send.at[t, k],
            recv_sem=ici_recv.at[t, k], device_id=(c, direct[t][0]), device_id_type=MESH,
        )

    def fwd(k):
        at = rows_of(k, direct[0][1])
        return pltpu.make_async_remote_copy(
            src_ref=at, dst_ref=at, send_sem=fwd_send.at[k],
            recv_sem=fwd_recv.at[k], device_id=(c, direct[1][0]), device_id_type=MESH,
        )

    def fwd_in(k):
        at = rows_of(k, sources[-1])
        return pltpu.make_async_remote_copy(
            src_ref=at, dst_ref=at, send_sem=fwd_send.at[k],
            recv_sem=fwd_recv.at[k], device_id=(c, direct[1][0]), device_id_type=MESH,
        )

    def across_core(t, k, who):
        at = rows_of(k, who[t])
        return pltpu.make_async_remote_copy(
            src_ref=at, dst_ref=at, send_sem=core_send.at[t, k],
            recv_sem=core_recv.at[t, k], device_id=(c, partner), device_id_type=MESH,
        )

    def to_peer(j, k):
        return pltpu.make_async_remote_copy(
            src_ref=update.at[k, peers[j][0]], dst_ref=arrived.at[j, :, k * WIDTH : (k + 1) * WIDTH],
            send_sem=z_send.at[j, k], recv_sem=z_recv.at[j, k],
            device_id=(peers[j][0], r), device_id_type=MESH,
        )

    def map_to_peer(j):
        return pltpu.make_async_remote_copy(
            src_ref=slots.at[peers[j][0]], dst_ref=slots_in.at[j],
            send_sem=map_send.at[j], recv_sem=map_recv.at[j],
            device_id=(peers[j][0], r), device_id_type=MESH,
        )

    sent = []

    def start(copy):
        copy.start()
        sent.append(copy)

    def send_own(k):
        for t in range(len(direct)):
            start(ici(t, k))
        start(across_core(0, k, sources))

    def relay(k):
        for t in range(len(direct)):
            ici_in(t, k).wait_recv()
            if forward and t == 0:
                start(fwd(k))
            start(across_core(t + 1, k, sources))

    def keep(k):
        return pltpu.make_async_copy(
            update.at[k, c], arrived.at[len(peers), :, k * WIDTH : (k + 1) * WIDTH],
            keep_sem.at[k],
        )

    def part(k, source):
        at = pl.ds(pl.multiple_of(source * block, block), block)
        return dot(coupling[:, at], gathered[k, at, :])

    def last_arrivals(k):
        if forward:
            fwd_in(k).wait_recv()
            start(across_core(len(sources) - 1, k, sources))

    def multiply_as_it_comes(k):
        ready = sources[: len(direct) + 1]
        total[...] = part(k, ready[0])
        for source in ready[1:]:
            total[...] += part(k, source)
        for t in range(len(direct) + 1):
            across_core(t, k, other).wait_recv()
            total[...] += part(k, other[t])
        last_arrivals(k)
        if forward:
            total[...] += part(k, sources[-1])
            across_core(len(other) - 1, k, other).wait_recv()
            total[...] += part(k, other[-1])
        coupled[...] = total[...].astype(jnp.bfloat16)

    def multiply(k):
        last_arrivals(k)
        for t in range(len(sources)):
            across_core(t, k, other).wait_recv()
        depth = gathered.shape[1]
        piece = min(DEPTH, depth)
        value = dot(coupling[:, :piece], gathered[k, :piece, :])
        if depth > piece:
            def more(b, acc):
                at = pl.ds(pl.multiple_of(b * piece, piece), piece)
                return acc + dot(coupling[:, at], gathered[k, at, :])

            value = lax.fori_loop(1, depth // piece, more, value)
        coupled[...] = value.astype(jnp.bfloat16)

    def finish(k):
        for i in range(leaves):
            rows = slice(i * leaf, (i + 1) * leaf)
            value = local_part[rows, k * WIDTH : (k + 1) * WIDTH] + dot(
                u[rows, :], coupled[i * rank : (i + 1) * rank, :]
            )
            update[k, i] = value.astype(jnp.bfloat16)
        for j in range(len(peers)):
            start(to_peer(j, k))
        keep(k).start()

    loads[0].wait()
    loads[1].wait()
    project(0, 1)
    pl.semaphore_wait(barrier, len(direct) + 1 + len(peers))
    send_own(0)
    for j in range(len(peers)):
        start(map_to_peer(j))
    keep_slots = pltpu.make_async_copy(
        slots.at[c], slots_in.at[len(peers)], keep_sem.at[chunks]
    )
    keep_slots.start()
    loads[2].wait()
    if chunks > 1:
        project(1, chunks)
    for load in loads[3:]:
        load.wait()
    for i in range(leaves):
        rows = slice(i * leaf, (i + 1) * leaf)
        local_part[rows, :] = dot(diag[i], omega[rows, :])
    send_own(1)
    relay(0)
    send_own(2)
    for k in range(chunks):
        if k + 1 < chunks:
            relay(k + 1)
            if k + 3 < chunks:
                send_own(k + 3)
        if k in (0, chunks - 1):
            multiply_as_it_comes(k)
        else:
            multiply(k)
        finish(k)
    for j in range(len(peers)):
        map_to_peer(j).wait_recv()
    keep_slots.wait()
    for copy in sent:
        copy.wait_send()
    for k in range(chunks):
        keep(k).wait()
        for j in range(len(peers)):
            to_peer(j, k).wait_recv()


def combine(arrived, slots, out_ref):
    half = out_ref.shape[1]
    for j in range(arrived.shape[0]):
        value = arrived[j].astype(jnp.float32)
        low, high = value[:half], value[half:]
        s0, s1 = slots[j, 0:1, :], slots[j, 4:5, :]
        for q in range(3):
            term = jnp.where(s0 == float(q), low, jnp.where(s1 == float(q), high, 0.0))
            out_ref[q] = term if j == 0 else out_ref[q] + term


def solution(mesh):
    n_child, n_rows = mesh.shape["child"], mesh.shape["rows"]

    def on_device(omega, leaf_diag, leaf_u, leaf_v, coupling, child_map):
        leaves, leaf = leaf_diag.shape[1], leaf_diag.shape[2]
        rank, samples = leaf_u.shape[2], omega.shape[2]
        chunks = samples // WIDTH
        block, depth = coupling.shape[1], coupling.shape[2]
        chips = n_rows // 2
        direct = 2 if chips == 4 else chips - 1
        everyone = 1 + direct + (chips == 4)
        peers = n_child - 1
        vmem = pltpu.VMEM
        bf16, f32 = jnp.bfloat16, jnp.float32
        dma = pltpu.SemaphoreType.DMA
        anywhere = pl.BlockSpec(memory_space=pl.ANY)
        arrived, slots = pl.pallas_call(
            functools.partial(kernel, n_child, n_rows),
            out_shape=[
                jax.ShapeDtypeStruct((n_child, leaf, samples), bf16),
                jax.ShapeDtypeStruct((n_child, 8, samples), f32),
            ],
            in_specs=[anywhere] * 2 + [pl.BlockSpec(memory_space=pltpu.SMEM)] + [anywhere] * 3,
            out_specs=[anywhere] * 2,
            scratch_shapes=[
                vmem((leaves * leaf, samples), bf16),
                vmem((leaves * leaf, rank), bf16),
                vmem((leaves, leaf, leaf), bf16),
                vmem((leaves * leaf, rank), bf16),
                vmem((block, depth), bf16),
                vmem((chunks, depth, WIDTH), bf16),
                vmem((leaves * leaf, samples), f32),
                vmem((block, WIDTH), f32),
                vmem((block, WIDTH), bf16),
                vmem((chunks, leaves, leaf, WIDTH), bf16),
                vmem((leaves, 8, samples), f32),
                dma((6,)),
                dma((direct, chunks)),
                dma((direct, chunks)),
                dma((chunks,)),
                dma((chunks,)),
                dma((everyone, chunks)),
                dma((everyone, chunks)),
                dma((peers, chunks)),
                dma((peers, chunks)),
                dma((peers,)),
                dma((peers,)),
                dma((chunks + 1,)),
            ],
            compiler_params=pltpu.CompilerParams(
                collective_id=0, has_side_effects=True, vmem_limit_bytes=60000 * 1024
            ),
        )(omega, leaf_v, child_map, leaf_diag, leaf_u, coupling)
        width = samples // STEPS
        return pl.pallas_call(
            combine,
            grid=(STEPS,),
            out_shape=jax.ShapeDtypeStruct((3, leaf // 2, samples), f32),
            in_specs=[
                pl.BlockSpec((n_child, leaf, width), lambda i: (0, 0, i)),
                pl.BlockSpec((n_child, 8, width), lambda i: (0, 0, i)),
            ],
            out_specs=pl.BlockSpec((3, leaf // 2, width), lambda i: (0, 0, i)),
        )(arrived, slots)

    placed = (
        P("child", "rows", None),
        P("child", "rows", None, None),
        P("child", "rows", None),
        P("child", "rows", None),
        P("child", "rows", None),
        P("child", "rows"),
    )
    return jax.shard_map(
        on_device,
        mesh=mesh,
        in_specs=placed,
        out_specs=P(None, ("child", "rows"), None),
        check_vma=False,
    )
```
